512 devices in a mesh: subj: 2 (over y), row: 16 (over x, core), col: 16 (over z).
Axes of the slice: x: 8, y: 2, z: 16, core: 2. Of those that a mesh axis runs over, the one named last changes fastest.
The devices are a block of a 8x8x16 slice.
Arguments:
- series: float32 [800, 65536], P(None, ('subj', 'row', 'col')), parts along dimension 1, as said below
- keep_mask: int32 [512, 256], P(('subj', 'row'), 'col'), parts along dimension 0, may hold values from 0 to 1, as said below
- row_owner: int32 [512], P('subj'), parts along dimension 0, may hold values from 0 to 15, as said below
Outputs:
- owned_tiles: bfloat16 [32, 16, 96, 128, 128], P(('subj', 'row'), 'col'), parts along dimension 0
- owned_ids: int32 [32, 16, 96], P(('subj', 'row'), 'col'), parts along dimension 0
The draws below stay inside these ranges and needn't reach their ends.
There are 2 independent parts, one for each index of `subj`. The reference program is written for one: setup_inputs(seed, part) draws one part's arguments, and reference() takes and returns one part's arrays. A program takes and returns all parts, laid end to end along the dimension named above; each array names one. Nothing has to cross between parts.
Inputs may be any that keep to these rules, and one draw needn't show every extreme that they name: Each voxel's series varies over time. `keep_mask`: of the 16 tiles that one tile row has in one column block, at most 6 are kept; in every draw one owner keeps exactly 6 in each of its tile rows in some column block. `row_owner`: the 16 tile rows of a row block have 16 different owners, and every owner holds 16 tile rows, from 16 different row blocks.
All inputs are finite; a program needn't handle non-finite values.
Results may differ from the reference program's by a relative error of at most 0.0042.
Values may be sent and summed in bfloat16 or wider, within the bound.
A program may use at most 64 MiB of HBM per device.

```python
import math
import jax
import jax.numpy as jnp
from jax import lax

TRS = 800
TILE = 128
CH = 128
NVOX = 32768
NTILES = 256
RT = 16
CT = 16
CAP = 6
RCAP = 96
N_ROW = 16
N_COL = 16


latent_count = 128


def draw_series(key, part):
    subkeys = jax.random.split(key, 6)
    latent = jax.random.normal(subkeys[0], (TRS, latent_count), jnp.float32)
    loadings = 1.2 / math.sqrt(latent_count) * jax.random.normal(subkeys[1], (latent_count, NVOX), jnp.float32)
    tr_scale = jnp.exp(jax.random.uniform(subkeys[4], (TRS, 1), jnp.float32, 0.0, math.log(1.2)))
    offset = jax.random.uniform(subkeys[5], (1, NVOX), jnp.float32, -5.0, 5.0)
    noise_part = jax.random.normal(subkeys[2], (TRS, NVOX), jnp.float32)
    vox_scale = jnp.exp(jax.random.uniform(subkeys[3], (1, NVOX), jnp.float32, 0.0, math.log(10.0)))
    signal = jnp.dot(latent, loadings) + noise_part
    return (offset + vox_scale * tr_scale * signal).astype(jnp.float32)


def routing(key):
    base_key = jax.random.fold_in(key, 7)
    row_blocks = NTILES // RT
    col_blocks = NTILES // CT
    owner_order = jax.random.permutation(jax.random.fold_in(base_key, 1), row_blocks)
    shifts = jax.vmap(lambda subkey: jax.random.permutation(subkey, RT))(jax.random.split(jax.random.fold_in(base_key, 2), row_blocks))
    block_ids = jnp.arange(row_blocks, dtype=jnp.int32)[:, None]
    owners = owner_order[(block_ids + shifts) % row_blocks].reshape(NTILES).astype(jnp.int32)
    load_level = jax.random.randint(jax.random.fold_in(base_key, 3), (row_blocks,), 0, 3)
    slot_draw = jax.random.randint(jax.random.fold_in(base_key, 4), (NTILES, col_blocks), 0, CAP + 1)
    slot_limit = jnp.minimum(CAP, slot_draw * (1 + load_level[owners])[:, None] // 2)
    forced = (owners == owner_order[0])[:, None] & (jnp.arange(col_blocks) == 0)[None, :]
    slot_limit = jnp.where(forced, CAP, slot_limit)
    tile_ranks = jax.vmap(lambda subkey: jax.random.permutation(subkey, CT))(jax.random.split(jax.random.fold_in(base_key, 5), NTILES * col_blocks))
    tile_ranks = tile_ranks.reshape(NTILES, col_blocks, CT)
    kept = (tile_ranks < slot_limit[:, :, None]).astype(jnp.int32).reshape(NTILES, NTILES)
    return (kept, owners)


def draw_keep_mask(key, part):
    kept, owners = routing(key)
    return kept


def draw_row_owner(key, part):
    kept, owners = routing(key)
    return owners


def setup_inputs(seed: int = 0, part: int = 0) -> dict:
    key_of = jax.random.split(jax.random.key(seed), 4)
    part_keys = jax.random.split(jax.random.fold_in(key_of[3], part), 4)
    series = draw_series(jax.random.fold_in(jax.random.fold_in(key_of[3], part), 71), part)
    keep_mask = draw_keep_mask(jax.random.fold_in(jax.random.fold_in(key_of[3], part), 71), part)
    row_owner = draw_row_owner(jax.random.fold_in(jax.random.fold_in(key_of[3], part), 71), part)
    return {"series": series, "keep_mask": keep_mask, "row_owner": row_owner}


epsilon = 1e-05

def reference(series, keep_mask, row_owner):
    average = lax.optimization_barrier(jnp.mean(series, axis=0, keepdims=True))
    centred = series - average
    spread = lax.optimization_barrier(jnp.mean(centred * centred, axis=0, keepdims=True))
    scored = (centred * lax.rsqrt(spread + epsilon)).astype(jnp.bfloat16)
    reordered = scored.reshape(TRS, N_ROW, N_COL, CH).transpose(0, 2, 1, 3).reshape(TRS, NVOX)
    row_tiles = scored.reshape(TRS, NTILES, TILE)
    col_tiles = reordered.reshape(TRS, NTILES, TILE)
    positions = jnp.arange(NTILES * CT, dtype=jnp.int32)
    slot_index = jnp.arange(RCAP, dtype=jnp.int32)

    def one_group(group_index):
        target = group_index // N_COL
        column_block = group_index % N_COL
        block_keep = lax.dynamic_slice_in_dim(keep_mask, (column_block * CT).astype(jnp.int32), CT, 1)
        owned = (row_owner == target).astype(jnp.int32)
        keep_flags = (block_keep * owned[:, None]).reshape(NTILES * CT)
        running = jnp.cumsum(keep_flags)
        slot_hit = (keep_flags[None, :] == 1) & (running[None, :] == slot_index[:, None] + 1)
        picked = lax.optimization_barrier(jnp.sum(jnp.where(slot_hit, positions[None, :], 0), axis=1)).astype(jnp.int32)
        present = running[-1] > slot_index
        row_ids = (picked // CT).astype(jnp.int32)
        col_ids = (column_block * CT + picked % CT).astype(jnp.int32)
        left_tiles = jnp.take(row_tiles, row_ids, axis=1).astype(jnp.float32)
        right_tiles = jnp.take(col_tiles, col_ids, axis=1).astype(jnp.float32)
        products = jnp.einsum('tsa,tsb->sab', left_tiles, right_tiles) * (1.0 / TRS)
        slot_tiles = jnp.where(present[:, None, None], products, 0.0).astype(jnp.bfloat16)
        slot_ids = jnp.where(present, row_ids * NTILES + col_ids, -1).astype(jnp.int32)
        return (slot_tiles, slot_ids)
    slot_tiles, slot_ids = lax.map(one_group, jnp.arange(N_ROW * N_COL, dtype=jnp.int32))
    return (slot_tiles.reshape(N_ROW, N_COL, RCAP, TILE, TILE), slot_ids.reshape(N_ROW, N_COL, RCAP))
```

```python
import functools

import jax
import jax.numpy as jnp
from jax import lax
from jax.experimental import pallas as pl
from jax.experimental.pallas import tpu as pltpu
from jax.sharding import PartitionSpec as P

MESH = pl.DeviceIdType.MESH
EPSILON = 1e-05
UNIT = 16
GROUPS = 2
PIECES = 4


def cut(first, size, parts):
    units = size // UNIT
    edges = [first + UNIT * (units * p // parts) for p in range(parts)] + [first + size]
    return [(a, b - a) for a, b in zip(edges[:-1], edges[1:])]


def move(
    rows,
    cols,
    groups,
    series_ref,
    keep_ref,
    owner_ref,
    left_ref,
    right_ref,
    flags_ref,
    *scratch,
):
    gathered, outbox = scratch[: len(groups)], scratch[len(groups) : 2 * len(groups)]
    keeps = scratch[2 * len(groups)]
    z_send, z_recv, x_send, x_recv, d_send, d_recv, a_send, a_recv, e_send, e_recv, k_send, k_recv = scratch[
        2 * len(groups) + 1 :
    ]
    chips = rows // 2
    row, col = lax.axis_index("row"), lax.axis_index("col")
    core, chip = lax.rem(row, 2), lax.div(row, 2)
    up, down = lax.rem(col + 1, cols), lax.rem(col + cols - 1, cols)
    partner = row + 1 - 2 * core

    def chip_at(offset):
        return lax.rem(chip + offset + chips, chips)

    def col_at(offset):
        return lax.rem(col + offset + cols, cols)

    def copy(src, dst, send, recv, to_row, to_col):
        return pltpu.make_async_remote_copy(
            src_ref=src,
            dst_ref=dst,
            send_sem=send,
            recv_sem=recv,
            device_id={"row": to_row, "col": to_col},
            device_id_type=MESH,
        )

    barrier = pltpu.get_barrier_semaphore()
    for offset in range(1, rows):
        pl.semaphore_signal(
            barrier, inc=1, device_id={"row": lax.rem(row + offset, rows), "col": col}, device_id_type=MESH
        )
    for to_col in (up, down):
        pl.semaphore_signal(barrier, inc=1, device_id={"row": row, "col": to_col}, device_id_type=MESH)

    frames = series_ref.shape[0]
    series = series_ref[...]
    centred = series - jnp.sum(series, axis=0, keepdims=True) * (1.0 / frames)
    spread = jnp.sum(centred * centred, axis=0, keepdims=True) * (1.0 / frames)
    scored = (centred * lax.rsqrt(spread + EPSILON)).astype(jnp.bfloat16)
    for g, pieces in enumerate(groups):
        first, size = pieces[0][0], sum(s for _, s in pieces)
        gathered[g][col] = scored[first : first + size]
    right_ref[row] = scored
    keeps[row] = keep_ref[...]

    pl.semaphore_wait(barrier, rows + 1)

    z_pieces = [(g, i, *piece) for g, pieces in enumerate(groups) for i, piece in enumerate(pieces)]
    x_pieces = [(pieces[0][0], sum(s for _, s in pieces)) for pieces in groups]

    def z_hops(n, way):
        return cols // 2 if n % 2 == way else cols - 1 - cols // 2

    def x_hops(n, way):
        return chips // 2 if n % 2 == way else chips - 1 - chips // 2

    def z_copy(n, way, hop):
        g, _, first, size = z_pieces[n]
        origin = col_at(1 - hop if way == 0 else hop - 1)
        part = gathered[g].at[origin, pl.ds(first - groups[g][0][0], size)]
        return copy(part, part, z_send.at[n, way, hop - 1], z_recv.at[n, way, hop - 1], row, up if way == 0 else down)

    def x_copy(n, way, hop):
        first, size = x_pieces[n]
        origin = 2 * chip_at(1 - hop if way == 0 else hop - 1) + core
        part = right_ref.at[origin, pl.ds(first, size)]
        to_row = 2 * chip_at(1 if way == 0 else -1) + core
        return copy(part, part, x_send.at[n, way, hop - 1], x_recv.at[n, way, hop - 1], to_row, col)

    def d_copy(n, offset):
        first, size = x_pieces[n]
        part = right_ref.at[2 * chip_at(offset) + core, pl.ds(first, size)]
        return copy(part, part, d_send.at[n, offset], d_recv.at[n, offset], partner, col)

    def k_copy(offset):
        return copy(
            keep_ref, keeps.at[row], k_send.at[offset], k_recv.at[offset], lax.rem(row + offset, rows), col
        )

    def z_start(g):
        for n, piece in enumerate(z_pieces):
            if piece[0] == g:
                for way in range(2):
                    z_copy(n, way, 1).start()

    def z_step(g, hop):
        for n, piece in enumerate(z_pieces):
            if piece[0] == g:
                for way in range(2):
                    if hop <= z_hops(n, way):
                        z_copy(n, way, hop).wait_recv()
                        if hop < z_hops(n, way):
                            z_copy(n, way, hop + 1).start()

    def x_step(hop):
        for n in range(len(x_pieces)):
            for way in range(2):
                if hop <= x_hops(n, way):
                    x_copy(n, way, hop).wait_recv()
                    if hop < x_hops(n, way):
                        x_copy(n, way, hop + 1).start()
                    d_copy(n, chips - hop if way == 0 else hop).start()

    same = lax.rem(col, 2) == 0
    to_core = lax.rem(row + col, 2)
    offsets = [0] + sorted(range(1, chips), key=lambda o: (min(o, chips - o), o))
    to_up = offsets[::2]

    def a_copy(g, offset):
        first, size = groups[g][0][0], sum(s for _, s in groups[g])
        return copy(
            outbox[g].at[offset],
            left_ref.at[row, pl.ds(first, size)],
            a_send.at[g, offset],
            a_recv.at[g, offset],
            2 * chip_at(offset) + to_core,
            col,
        )

    def picked(offset):
        owner = 2 * chip_at(offset) + to_core
        place = jnp.int32(0)
        for i in range(cols):
            place = jnp.where(owner_ref[row * cols + i] == owner, i, place)
        return place

    def a_start(g):
        first, size = groups[g][0][0], sum(s for _, s in groups[g])
        for offset in offsets[1:] + [0]:
            place = picked(offset)
            if offset:
                outbox[g][offset] = gathered[g][place]
                a_copy(g, offset).start()
            else:

                @pl.when(same)
                def _():
                    left_ref[row, pl.ds(first, size)] = gathered[g][place]

                @pl.when(jnp.logical_not(same))
                def _():
                    outbox[g][offset] = gathered[g][place]
                    a_copy(g, offset).start()

    def e_copy(g, offset):
        first, size = groups[g][0][0], sum(s for _, s in groups[g])
        part = left_ref.at[2 * chip_at(-offset) + to_core, pl.ds(first, size)]
        return copy(part, part, e_send.at[g, offset], e_recv.at[g, offset], row, up if offset in to_up else down)

    def e_start(g):
        for offset in offsets:
            if offset:
                a_copy(g, offset).wait_recv()
            else:

                @pl.when(jnp.logical_not(same))
                def _():
                    a_copy(g, offset).wait_recv()

            e_copy(g, offset).start()

    last = cols // 2
    z_start(0)
    for n in range(len(x_pieces)):
        for way in range(2):
            x_copy(n, way, 1).start()
    for offset in range(1, rows):
        k_copy(offset).start()
    for n in range(len(x_pieces)):
        d_copy(n, 0).start()
    for g in range(len(groups)):
        for hop in range(1, last):
            z_step(g, hop)
            if g == 0 and hop % 2 == 0:
                x_step(hop // 2)
        if g + 1 < len(groups):
            z_start(g + 1)
        z_step(g, last)
        if g == 0:
            for hop in range(last // 2, chips // 2 + 1):
                x_step(hop)
        a_start(g)
        if g:
            e_start(g - 1)
    e_start(len(groups) - 1)

    for offset in range(1, rows):
        k_copy(offset).wait_recv()
    for k in range(rows):
        place = jnp.int32(0)
        for i in range(cols):
            place = jnp.where(owner_ref[k * cols + i] == row, i, place)
        flags_ref[pl.ds(k, 1), :] = keeps[k, pl.ds(place, 1), :]
    for n in range(len(x_pieces)):
        for offset in range(chips):
            d_copy(n, offset).wait_recv()
    for g in range(len(groups)):
        for offset in range(chips):
            e_copy(g, offset).wait_recv()

    for n in range(len(z_pieces)):
        for way in range(2):
            for hop in range(1, z_hops(n, way) + 1):
                z_copy(n, way, hop).wait_send()
    for n in range(len(x_pieces)):
        for way in range(2):
            for hop in range(1, x_hops(n, way) + 1):
                x_copy(n, way, hop).wait_send()
        for offset in range(chips):
            d_copy(n, offset).wait_send()
    for offset in range(1, rows):
        k_copy(offset).wait_send()
    for g in range(len(groups)):
        for offset in range(chips):
            if offset:
                a_copy(g, offset).wait_send()
            else:

                @pl.when(jnp.logical_not(same))
                def _():
                    a_copy(g, offset).wait_send()

            e_copy(g, offset).wait_send()


def multiply(capacity, limit, left_ref, right_ref, flags_ref, owner_ref, tiles_ref, ids_ref, packed, ids, places, sem):
    rows, frames, tile = left_ref.shape
    cols = flags_ref.shape[1]
    row, col = lax.axis_index("row"), lax.axis_index("col")
    total_cols = cols * lax.axis_size("col")
    first_col = col * cols
    for i in range(cols + 1):
        places[i] = 0

    def one_row(k, start):
        count = jnp.int32(0)
        for j in range(cols):
            places[count] = j
            count += flags_ref[k, j]
        place = jnp.int32(0)
        for i in range(cols):
            place = jnp.where(owner_ref[k * cols + i] == row, i, place)
        base = (k * cols + place) * total_cols + first_col
        rows_of = left_ref[k]
        for s in range(0, limit, 2):
            a, b = places[s], places[s + 1]
            product = lax.dot_general(
                rows_of,
                jnp.concatenate([right_ref[a], right_ref[b]], axis=1),
                (((0,), (0,)), ((), ())),
                preferred_element_type=jnp.float32,
            ) * (1.0 / frames)
            packed[start + s] = product[:, :tile].astype(packed.dtype)
            packed[start + s + 1] = product[:, tile:].astype(packed.dtype)
            ids[start + s] = base + a
            ids[start + s + 1] = base + b
        return start + count

    total = lax.fori_loop(0, rows, one_row, jnp.int32(0))

    def blank(s, carry):
        packed[s] = jnp.zeros_like(packed[s])
        ids[s] = -1
        return carry

    lax.fori_loop(total, capacity, blank, 0)
    out = pltpu.make_async_copy(packed.at[pl.ds(0, capacity)], tiles_ref, sem)
    out.start()
    for s in range(capacity):
        ids_ref[s] = ids[s]
    out.wait()


def shards(series, keep_mask, row_owner):
    frames, tile = series.shape
    row_count, col_count = keep_mask.shape
    rows, cols = lax.axis_size("row"), lax.axis_size("col")
    limit = max(2, 3 * col_count // 8)
    capacity = row_count * limit
    groups = [cut(first, size, PIECES) for first, size in cut(0, frames, GROUPS)]
    sizes = [sum(s for _, s in pieces) for pieces in groups]
    n_z, n_g = sum(len(pieces) for pieces in groups), len(groups)
    chips = rows // 2
    vmem, smem = pl.BlockSpec(memory_space=pltpu.VMEM), pl.BlockSpec(memory_space=pltpu.SMEM)
    dma = pltpu.SemaphoreType.DMA
    left, right, flags = pl.pallas_call(
        functools.partial(move, rows, cols, groups),
        out_shape=(
            jax.ShapeDtypeStruct((rows, frames, tile), jnp.bfloat16),
            jax.ShapeDtypeStruct((rows, frames, tile), jnp.bfloat16),
            jax.ShapeDtypeStruct((rows, col_count), jnp.int32),
        ),
        in_specs=[vmem, vmem, smem],
        out_specs=(vmem, vmem, vmem),
        scratch_shapes=[
            *[pltpu.VMEM((cols, size, tile), jnp.bfloat16) for size in sizes],
            *[pltpu.VMEM((chips, size, tile), jnp.bfloat16) for size in sizes],
            pltpu.VMEM((rows, row_count, col_count), jnp.int32),
            *[dma((n_z, 2, cols // 2))] * 2,
            *[dma((n_g, 2, chips // 2))] * 2,
            *[dma((n_g, chips))] * 2,
            *[dma((n_g, chips))] * 2,
            *[dma((n_g, chips))] * 2,
            *[dma((rows,))] * 2,
        ],
        compiler_params=pltpu.CompilerParams(collective_id=0, has_side_effects=True, vmem_limit_bytes=24 * 2**20),
    )(series, keep_mask, row_owner)
    tiles, ids = pl.pallas_call(
        functools.partial(multiply, capacity, limit),
        out_shape=(
            jax.ShapeDtypeStruct((capacity, tile, tile), jnp.bfloat16),
            jax.ShapeDtypeStruct((capacity,), jnp.int32),
        ),
        in_specs=[vmem, vmem, smem, smem],
        out_specs=(pl.BlockSpec(memory_space=pl.ANY), smem),
        scratch_shapes=[
            pltpu.VMEM((capacity + limit, tile, tile), jnp.bfloat16),
            pltpu.SMEM((capacity + limit,), jnp.int32),
            pltpu.SMEM((col_count + 1,), jnp.int32),
            dma(()),
        ],
        compiler_params=pltpu.CompilerParams(vmem_limit_bytes=24 * 2**20),
    )(left, right, flags, row_owner)
    return tiles.reshape(1, 1, capacity, tile, tile), ids.reshape(1, 1, capacity)


def solution(mesh):
    in_specs = (P(None, ("subj", "row", "col")), P(("subj", "row"), "col"), P("subj"))
    out_specs = (P(("subj", "row"), "col", None, None, None), P(("subj", "row"), "col", None))
    return jax.shard_map(shards, mesh=mesh, in_specs=in_specs, out_specs=out_specs, check_vma=False)
```

```python
import functools

import jax
import jax.numpy as jnp
from jax import lax
from jax.experimental import pallas as pl
from jax.experimental.pallas import tpu as pltpu
from jax.sharding import PartitionSpec as P

MESH = pl.DeviceIdType.MESH
EPSILON = 1e-05
UNIT = 16
GROUPS = 4
X_PIECES = 2
BEHIND = 6
STEP, HOP, BLOCK = 2.6, 2.6, 4.4


def cut(first, size, parts):
    units = size // UNIT
    edges = [first + UNIT * (units * p // parts) for p in range(parts)] + [first + size]
    return [(a, b - a) for a, b in zip(edges[:-1], edges[1:])]


def arrivals(cols, chips, behind, ahead):
    last = cols - 1
    start = [STEP * c + 4.0 for c in range(cols)]
    up = [[1e9] * (behind + 1) for _ in range(cols)]
    down = [[1e9] * (ahead + 1) for _ in range(cols)]
    for _ in range(4 * cols):
        for c in range(cols):
            above, below = (c + 1) % cols, (c - 1) % cols
            for i in range(1, ahead + 1):
                ready = start[above] if i == 1 else down[above][i - 1]
                if above == 0:
                    ready = max(ready, up[0][1])
                queue = down[c][i - 1] - HOP + BLOCK if i > 1 else 0.0
                down[c][i] = max(ready, queue) + HOP
            for h in range(1, behind + 1):
                if c == 0:
                    ready = start[cols - h]
                else:
                    ready = max(start[below] if h == 1 else up[below][h - 1], down[below][1] if below != last else 0.0)
                queue = up[c][h - 1] - HOP + BLOCK if h > 1 and c else 0.0
                up[c][h] = max(ready, queue) + HOP
    turns = []
    for c in range(cols):
        floor = 0 if c == last else 1
        from_behind = [max(floor, sum(down[c][i] <= up[c][h] for i in range(1, ahead + 1))) for h in range(1, behind + 1)]
        along = [sum(down[c][i] <= start[c] + BLOCK * h for i in range(1, ahead + 1)) for h in range(1, chips // 2 + 1)]
        for turn in (from_behind, along):
            for h in range(1, len(turn)):
                turn[h] = max(turn[h], turn[h - 1])
        turns.append((from_behind, along))
    return turns


def move(
    rows,
    cols,
    groups,
    series_hbm,
    keep_hbm,
    owner_hbm,
    left_ref,
    right_ref,
    flags_ref,
    spots_ref,
    *scratch,
):
    n_g = len(groups)
    gathered, outbox = scratch[:n_g], scratch[n_g : 2 * n_g]
    series_ref, keep_ref, owner_ref, keeps, load = scratch[2 * n_g : 2 * n_g + 5]
    (
        up_send,
        up_recv,
        down_send,
        down_recv,
        far_send,
        x_send,
        x_recv,
        d_send,
        d_recv,
        a_send,
        a_recv,
        e_send,
        e_recv,
        f_send,
        k_send,
        k_recv,
    ) = scratch[2 * n_g + 5 :]
    chips = rows // 2
    row, col = lax.axis_index("row"), lax.axis_index("col")
    core, chip = lax.rem(row, 2), lax.div(row, 2)
    last = cols - 1
    behind = BEHIND
    ahead = cols - 1 - behind
    above, below = lax.rem(col + 1, cols), lax.rem(col + cols - 1, cols)
    partner = row + 1 - 2 * core
    is_first, is_last = col == 0, col == last

    def when(condition, do):
        pl.when(condition)(do)

    def chip_at(offset):
        return lax.rem(chip + offset + chips, chips)

    def col_at(offset):
        return lax.rem(col + offset + cols, cols)

    def greet(to_row, to_col):
        pl.semaphore_signal(
            pltpu.get_barrier_semaphore(), inc=1, device_id={"row": to_row, "col": to_col}, device_id_type=MESH
        )

    def copy(src, dst, send, recv, to_row, to_col):
        return pltpu.make_async_remote_copy(
            src_ref=src,
            dst_ref=dst,
            send_sem=send,
            recv_sem=recv,
            device_id={"row": to_row, "col": to_col},
            device_id_type=MESH,
        )

    loads = [
        pltpu.make_async_copy(src, dst, load.at[i])
        for i, (src, dst) in enumerate(((series_hbm, series_ref), (owner_hbm, owner_ref), (keep_hbm, keep_ref)))
    ]
    for one in loads:
        one.start()

    barrier = pltpu.get_barrier_semaphore()
    greet(2 * chip_at(1) + core, col)
    greet(2 * chip_at(-1) + core, col)
    greet(partner, col)
    pl.when(is_first)(lambda: greet(row, last))

    loads[0].wait()
    frames = series_ref.shape[0]
    series = series_ref[...]
    centred = series - jnp.sum(series, axis=0, keepdims=True) * (1.0 / frames)
    spread = jnp.sum(centred * centred, axis=0, keepdims=True) * (1.0 / frames)
    scored = (centred * lax.rsqrt(spread + EPSILON)).astype(jnp.bfloat16)
    for g, (first, size) in enumerate(groups):
        gathered[g][col] = scored[first : first + size]
    right_ref[row] = scored

    pl.semaphore_wait(barrier, 4 - jnp.where(is_first, 1, 0) + jnp.where(is_last, 1, 0))
    pl.when(jnp.logical_not(is_last))(lambda: greet(row, above))

    x_pieces = cut(0, frames, X_PIECES)

    def up_copy(g, hop):
        part = gathered[g].at[col_at(1 - hop)]
        return copy(part, part, up_send.at[g, hop - 1], up_recv.at[g, hop - 1], row, above)

    def down_copy(g, hop):
        part = gathered[g].at[col_at(hop - 1)]
        return copy(part, part, down_send.at[g, hop - 1], down_recv.at[g, hop - 1], row, below)

    def far_copy(g, hop):
        part = gathered[g].at[col]
        return copy(part, part, far_send.at[g], up_recv.at[g, hop - 1], row, 0)

    def x_hops(n, way):
        return chips // 2 if n % 2 == way else chips - 1 - chips // 2

    def x_copy(n, way, hop):
        first, size = x_pieces[n]
        origin = 2 * chip_at(1 - hop if way == 0 else hop - 1) + core
        part = right_ref.at[origin, pl.ds(first, size)]
        to_row = 2 * chip_at(1 if way == 0 else -1) + core
        return copy(part, part, x_send.at[n, way, hop - 1], x_recv.at[n, way, hop - 1], to_row, col)

    def d_copy(n, offset):
        first, size = x_pieces[n]
        part = right_ref.at[2 * chip_at(offset) + core, pl.ds(first, size)]
        return copy(part, part, d_send.at[n, offset], d_recv.at[n, offset], partner, col)

    def k_copy(offset):
        return copy(keep_ref, keeps.at[row], k_send.at[offset], k_recv.at[offset], lax.rem(row + offset, rows), col)

    turns = arrivals(cols, chips, behind, ahead)
    held = turns[0][0][0]

    def up_step(hop):
        for g in range(n_g):
            up_copy(g, hop).wait_recv()
            if hop < behind:
                pl.when(jnp.logical_not(is_last))(lambda: up_copy(g, hop + 1).start())
            if hop == 1:

                @pl.when(is_first)
                def _():
                    down_copy(g, 1).start()

        if hop == 1:

            @pl.when(is_first)
            def _():
                for i in range(1, min(held, ahead - 1) + 1):
                    for g in range(n_g):
                        down_copy(g, i + 1).start()

    def down_step(hop):
        for g in range(n_g):
            down_copy(g, hop).wait_recv()
            if hop < ahead:
                if hop <= held:
                    pl.when(jnp.logical_not(is_first))(lambda: down_copy(g, hop + 1).start())
                else:
                    down_copy(g, hop + 1).start()
            if hop == 1:
                pl.when(jnp.logical_not(is_last))(lambda: up_copy(g, 1).start())

    def x_step(hop):
        for n in range(len(x_pieces)):
            for way in range(2):
                if hop <= x_hops(n, way):
                    x_copy(n, way, hop).wait_recv()
                    if hop < x_hops(n, way):
                        x_copy(n, way, hop + 1).start()
                    d_copy(n, chips - hop if way == 0 else hop).start()

    for g in range(n_g):
        pl.when(is_last)(lambda: up_copy(g, 1).start())
        for hop in range(2, behind + 1):
            pl.when(col == cols - hop)(lambda: far_copy(g, hop).start())
    for g in range(n_g):
        pl.when(jnp.logical_not(is_first))(lambda: down_copy(g, 1).start())
    for n in range(len(x_pieces)):
        for way in range(2):
            x_copy(n, way, 1).start()
    for n in range(len(x_pieces)):
        d_copy(n, 0).start()

    same = lax.rem(col, 2) == 0
    to_core = lax.rem(row + col, 2)
    offsets = [0] + sorted(range(1, chips), key=lambda o: (min(o, chips - o), o))
    to_above = offsets[::2]
    loads[1].wait()
    loads[2].wait()

    def picked(k, owner):
        place = jnp.int32(0)
        for i in range(cols):
            place = jnp.where(owner_ref[k * cols + i] == owner, i, place)
        return place

    for turn in range(ahead + 1):
        if turn:
            down_step(turn)
        for hop in range(1, behind + 1):
            at = [c for c in range(cols) if turns[c][0][hop - 1] == turn]
            if at:
                pl.when(functools.reduce(jnp.logical_or, [col == c for c in at]))(functools.partial(up_step, hop))
        for hop in range(1, chips // 2 + 1):
            at = [c for c in range(cols) if turns[c][1][hop - 1] == turn]
            if at:
                pl.when(functools.reduce(jnp.logical_or, [col == c for c in at]))(functools.partial(x_step, hop))
    for n in range(len(x_pieces)):
        for offset in range(chips):
            d_copy(n, offset).wait_recv()

    def a_copy(g, offset):
        return copy(
            outbox[g].at[offset],
            left_ref.at[row, pl.ds(*groups[g])],
            a_send.at[g, offset],
            a_recv.at[g, offset],
            2 * chip_at(offset) + to_core,
            col,
        )

    places = [picked(row, 2 * chip_at(offset) + to_core) for offset in range(chips)]

    def a_start(g):
        for offset in offsets[1:]:
            outbox[g][offset] = gathered[g][places[offset]]
            a_copy(g, offset).start()

        @pl.when(same)
        def _():
            left_ref[row, pl.ds(*groups[g])] = gathered[g][places[0]]

        @pl.when(jnp.logical_not(same))
        def _():
            outbox[g][0] = gathered[g][places[0]]
            a_copy(g, 0).start()

    def e_copy(g, offset, to_col, send):
        part = left_ref.at[2 * chip_at(-offset) + to_core, pl.ds(*groups[g])]
        return copy(part, part, send.at[g, offset], e_recv.at[g, offset], row, to_col)

    def e_start(g):
        for offset in offsets:
            if offset:
                a_copy(g, offset).wait_recv()
            else:
                pl.when(jnp.logical_not(same))(lambda: a_copy(g, 0).wait_recv())
            if offset in to_above:
                pl.when(jnp.logical_not(is_last))(lambda: e_copy(g, offset, above, e_send).start())
                pl.when(col == 1)(lambda: e_copy(g, offset, below, f_send).start())
            else:
                e_copy(g, offset, below, e_send).start()

    for g in range(n_g):
        a_start(g)
        if g == 0:
            keeps[row] = keep_ref[...]
            for offset in range(1, rows):
                k_copy(offset).start()
    for g in range(n_g):
        e_start(g)

    for offset in range(1, rows):
        k_copy(offset).wait_recv()
    spots = jnp.zeros(spots_ref.shape, jnp.int32)
    lane = lax.broadcasted_iota(jnp.int32, spots_ref.shape, 1)
    for k in range(rows):
        place = picked(k, row)
        flags_ref[pl.ds(k, 1), :] = keeps[k, pl.ds(place, 1), :]
        spots = jnp.where(lane == k, place, spots)
    spots_ref[...] = spots
    for g in range(n_g):
        for offset in range(chips):
            e_copy(g, offset, above, e_send).wait_recv()

    for g in range(n_g):
        for hop in range(1, ahead + 1):
            down_copy(g, hop).wait_send()
        up_copy(g, 1).wait_send()
        for hop in range(2, behind + 1):
            pl.when(jnp.logical_not(is_last))(lambda: up_copy(g, hop).wait_send())
            pl.when(col == cols - hop)(lambda: far_copy(g, hop).wait_send())
    for n in range(len(x_pieces)):
        for way in range(2):
            for hop in range(1, x_hops(n, way) + 1):
                x_copy(n, way, hop).wait_send()
        for offset in range(chips):
            d_copy(n, offset).wait_send()
    for offset in range(1, rows):
        k_copy(offset).wait_send()
    for g in range(n_g):
        for offset in range(chips):
            if offset:
                a_copy(g, offset).wait_send()
            else:
                pl.when(jnp.logical_not(same))(lambda: a_copy(g, 0).wait_send())
            if offset in to_above:
                pl.when(jnp.logical_not(is_last))(lambda: e_copy(g, offset, above, e_send).wait_send())
                pl.when(col == 1)(lambda: e_copy(g, offset, below, f_send).wait_send())
            else:
                e_copy(g, offset, below, e_send).wait_send()


def multiply(capacity, limit, left_ref, right_ref, flags_ref, spots_ref, tiles_ref, ids_ref, packed, ids, places, sem):
    rows, frames, tile = left_ref.shape
    cols = flags_ref.shape[1]
    col = lax.axis_index("col")
    total_cols = cols * lax.axis_size("col")
    first_col = col * cols
    for i in range(cols + 1):
        places[i] = 0

    def one_row(k, start):
        count = jnp.int32(0)
        for j in range(cols):
            places[count] = j
            count += flags_ref[k, j]
        base = (k * cols + spots_ref[0, k]) * total_cols + first_col
        rows_of = left_ref[k]
        for s in range(0, limit, 2):
            a, b = places[s], places[s + 1]
            product = lax.dot_general(
                rows_of,
                jnp.concatenate([right_ref[a], right_ref[b]], axis=1),
                (((0,), (0,)), ((), ())),
                preferred_element_type=jnp.float32,
            ) * (1.0 / frames)
            packed[start + s] = product[:, :tile].astype(packed.dtype)
            packed[start + s + 1] = product[:, tile:].astype(packed.dtype)
            ids[start + s] = base + a
            ids[start + s + 1] = base + b
        return start + count

    total = lax.fori_loop(0, rows, one_row, jnp.int32(0))

    def blank(s, carry):
        packed[s] = jnp.zeros_like(packed[s])
        ids[s] = -1
        return carry

    lax.fori_loop(total, capacity, blank, 0)
    out = pltpu.make_async_copy(packed.at[pl.ds(0, capacity)], tiles_ref, sem)
    out.start()
    for s in range(capacity):
        ids_ref[s] = ids[s]
    out.wait()


def shards(series, keep_mask, row_owner):
    frames, tile = series.shape
    row_count, col_count = keep_mask.shape
    rows, cols = lax.axis_size("row"), lax.axis_size("col")
    limit = max(2, 3 * col_count // 8)
    capacity = row_count * limit
    groups = cut(0, frames, GROUPS)
    chips = rows // 2
    vmem, smem, hbm = (pl.BlockSpec(memory_space=m) for m in (pltpu.VMEM, pltpu.SMEM, pltpu.HBM))
    dma = pltpu.SemaphoreType.DMA
    left, right, flags, spots = pl.pallas_call(
        functools.partial(move, rows, cols, groups),
        out_shape=(
            jax.ShapeDtypeStruct((rows, frames, tile), jnp.bfloat16),
            jax.ShapeDtypeStruct((rows, frames, tile), jnp.bfloat16),
            jax.ShapeDtypeStruct((rows, col_count), jnp.int32),
            jax.ShapeDtypeStruct((1, rows), jnp.int32),
        ),
        in_specs=[hbm, hbm, hbm],
        out_specs=(vmem, vmem, vmem, vmem),
        scratch_shapes=[
            *[pltpu.VMEM((cols, size, tile), jnp.bfloat16) for _, size in groups],
            *[pltpu.VMEM((chips, size, tile), jnp.bfloat16) for _, size in groups],
            pltpu.VMEM((frames, tile), series.dtype),
            pltpu.VMEM((row_count, col_count), jnp.int32),
            pltpu.SMEM(row_owner.shape, jnp.int32),
            pltpu.VMEM((rows, row_count, col_count), jnp.int32),
            dma((3,)),
            *[dma((GROUPS, BEHIND))] * 2,
            *[dma((GROUPS, cols - 1 - BEHIND))] * 2,
            dma((GROUPS,)),
            *[dma((X_PIECES, 2, chips // 2))] * 2,
            *[dma((X_PIECES, chips))] * 2,
            *[dma((GROUPS, chips))] * 2,
            *[dma((GROUPS, chips))] * 3,
            *[dma((rows,))] * 2,
        ],
        compiler_params=pltpu.CompilerParams(collective_id=0, has_side_effects=True, vmem_limit_bytes=24 * 2**20),
    )(series, keep_mask, row_owner)
    tiles, ids = pl.pallas_call(
        functools.partial(multiply, capacity, limit),
        out_shape=(
            jax.ShapeDtypeStruct((capacity, tile, tile), jnp.bfloat16),
            jax.ShapeDtypeStruct((capacity,), jnp.int32),
        ),
        in_specs=[vmem, vmem, smem, smem],
        out_specs=(pl.BlockSpec(memory_space=pl.ANY), smem),
        scratch_shapes=[
            pltpu.VMEM((capacity + limit, tile, tile), jnp.bfloat16),
            pltpu.SMEM((capacity + limit,), jnp.int32),
            pltpu.SMEM((col_count + 1,), jnp.int32),
            dma(()),
        ],
        compiler_params=pltpu.CompilerParams(vmem_limit_bytes=24 * 2**20),
    )(left, right, flags, spots)
    return tiles.reshape(1, 1, capacity, tile, tile), ids.reshape(1, 1, capacity)


def solution(mesh):
    in_specs = (P(None, ("subj", "row", "col")), P(("subj", "row"), "col"), P("subj"))
    out_specs = (P(("subj", "row"), "col", None, None, None), P(("subj", "row"), "col", None))
    return jax.shard_map(shards, mesh=mesh, in_specs=in_specs, out_specs=out_specs, check_vma=False)
```

```python
import functools

import jax
import jax.numpy as jnp
from jax import lax
from jax.experimental import pallas as pl
from jax.experimental.pallas import tpu as pltpu
from jax.sharding import PartitionSpec as P

MESH = pl.DeviceIdType.MESH
EPSILON = 1e-05
RUN = 8
UNIT = 16
GROUPS = 2
PIECES = 4


def cut(first, size, parts):
    units = size // UNIT
    edges = [first + UNIT * (units * p // parts) for p in range(parts)] + [first + size]
    return [(a, b - a) for a, b in zip(edges[:-1], edges[1:])]


def move(
    rows,
    cols,
    groups,
    series_ref,
    keep_ref,
    owner_ref,
    left_ref,
    right_ref,
    flags_ref,
    *scratch,
):
    gathered, outbox = scratch[: len(groups)], scratch[len(groups) : 2 * len(groups)]
    keeps = scratch[2 * len(groups)]
    z_send, z_recv, x_send, x_recv, d_send, d_recv, a_send, a_recv, e_send, e_recv, k_send, k_recv = scratch[
        2 * len(groups) + 1 :
    ]
    chips = rows // 2
    row, col = lax.axis_index("row"), lax.axis_index("col")
    core, chip = lax.rem(row, 2), lax.div(row, 2)
    up, down = lax.rem(col + 1, cols), lax.rem(col + cols - 1, cols)
    partner = row + 1 - 2 * core

    def chip_at(offset):
        return lax.rem(chip + offset + chips, chips)

    def col_at(offset):
        return lax.rem(col + offset + cols, cols)

    def copy(src, dst, send, recv, to_row, to_col):
        return pltpu.make_async_remote_copy(
            src_ref=src,
            dst_ref=dst,
            send_sem=send,
            recv_sem=recv,
            device_id={"row": to_row, "col": to_col},
            device_id_type=MESH,
        )

    barrier = pltpu.get_barrier_semaphore()
    for offset in range(1, rows):
        pl.semaphore_signal(
            barrier, inc=1, device_id={"row": lax.rem(row + offset, rows), "col": col}, device_id_type=MESH
        )
    for to_col in (up, down):
        pl.semaphore_signal(barrier, inc=1, device_id={"row": row, "col": to_col}, device_id_type=MESH)

    frames = series_ref.shape[0]
    series = series_ref[...]
    centred = series - jnp.sum(series, axis=0, keepdims=True) * (1.0 / frames)
    spread = jnp.sum(centred * centred, axis=0, keepdims=True) * (1.0 / frames)
    scored = (centred * lax.rsqrt(spread + EPSILON)).astype(jnp.bfloat16)
    for g, pieces in enumerate(groups):
        first, size = pieces[0][0], sum(s for _, s in pieces)
        gathered[g][col] = scored[first : first + size]
    right_ref[row] = scored
    keeps[row] = keep_ref[...]

    pl.semaphore_wait(barrier, rows + 1)

    z_pieces = [(g, i, *piece) for g, pieces in enumerate(groups) for i, piece in enumerate(pieces)]
    x_pieces = [(pieces[0][0], sum(s for _, s in pieces)) for pieces in groups]

    def z_hops(n, way):
        return cols // 2 if n % 2 == way else cols - 1 - cols // 2

    def x_hops(n, way):
        return chips // 2 if n % 2 == way else chips - 1 - chips // 2

    def z_copy(n, way, hop):
        g, _, first, size = z_pieces[n]
        origin = col_at(1 - hop if way == 0 else hop - 1)
        part = gathered[g].at[origin, pl.ds(first - groups[g][0][0], size)]
        return copy(part, part, z_send.at[g], z_recv.at[n, way, hop - 1], row, up if way == 0 else down)

    def x_copy(n, way, hop):
        first, size = x_pieces[n]
        origin = 2 * chip_at(1 - hop if way == 0 else hop - 1) + core
        part = right_ref.at[origin, pl.ds(first, size)]
        to_row = 2 * chip_at(1 if way == 0 else -1) + core
        return copy(part, part, x_send.at[n], x_recv.at[n, way, hop - 1], to_row, col)

    def d_copy(n, offset):
        first, size = x_pieces[n]
        part = right_ref.at[2 * chip_at(offset) + core, pl.ds(first, size)]
        return copy(part, part, d_send.at[n], d_recv.at[n, offset], partner, col)

    def k_copy(offset):
        return copy(
            keep_ref, keeps.at[row], k_send.at[0], k_recv.at[offset], lax.rem(row + offset, rows), col
        )

    def z_start(g):
        for n, piece in enumerate(z_pieces):
            if piece[0] == g:
                for way in range(2):
                    z_copy(n, way, 1).start()

    def z_step(g, hop):
        for n, piece in enumerate(z_pieces):
            if piece[0] == g:
                for way in range(2):
                    if hop <= z_hops(n, way):
                        z_copy(n, way, hop).wait_recv()
                        if hop < z_hops(n, way):
                            z_copy(n, way, hop + 1).start()

    def x_step(hop):
        for n in range(len(x_pieces)):
            for way in range(2):
                if hop <= x_hops(n, way):
                    x_copy(n, way, hop).wait_recv()
                    if hop < x_hops(n, way):
                        x_copy(n, way, hop + 1).start()
                    d_copy(n, chips - hop if way == 0 else hop).start()

    same = lax.rem(col, 2) == 0
    to_core = lax.rem(row + col, 2)
    offsets = [0] + sorted(range(1, chips), key=lambda o: (min(o, chips - o), o))
    to_up = offsets[::2]

    def a_copy(g, offset):
        first, size = groups[g][0][0], sum(s for _, s in groups[g])
        return copy(
            outbox[g].at[offset],
            left_ref.at[row, pl.ds(first, size)],
            a_send.at[g],
            a_recv.at[g, offset],
            2 * chip_at(offset) + to_core,
            col,
        )

    def picked(offset):
        owner = 2 * chip_at(offset) + to_core
        place = jnp.int32(0)
        for i in range(cols):
            place = jnp.where(owner_ref[row * cols + i] == owner, i, place)
        return place

    def a_start(g):
        first, size = groups[g][0][0], sum(s for _, s in groups[g])
        for offset in offsets[1:] + [0]:
            place = picked(offset)
            if offset:
                outbox[g][offset] = gathered[g][place]
                a_copy(g, offset).start()
            else:

                @pl.when(same)
                def _():
                    left_ref[row, pl.ds(first, size)] = gathered[g][place]

                @pl.when(jnp.logical_not(same))
                def _():
                    outbox[g][offset] = gathered[g][place]
                    a_copy(g, offset).start()

    def e_copy(g, offset):
        first, size = groups[g][0][0], sum(s for _, s in groups[g])
        part = left_ref.at[2 * chip_at(-offset) + to_core, pl.ds(first, size)]
        return copy(part, part, e_send.at[g], e_recv.at[g, offset], row, up if offset in to_up else down)

    def e_start(g):
        for offset in offsets:
            if offset:
                a_copy(g, offset).wait_recv()
            else:

                @pl.when(jnp.logical_not(same))
                def _():
                    a_copy(g, offset).wait_recv()

            e_copy(g, offset).start()

    last = cols // 2
    z_start(0)
    for n in range(len(x_pieces)):
        for way in range(2):
            x_copy(n, way, 1).start()
    for offset in range(1, rows):
        k_copy(offset).start()
    for n in range(len(x_pieces)):
        d_copy(n, 0).start()
    for g in range(len(groups)):
        for hop in range(1, last):
            z_step(g, hop)
            if g == 0 and hop % 2 == 0:
                x_step(hop // 2)
        if g + 1 < len(groups):
            z_start(g + 1)
        z_step(g, last)
        if g == 0:
            for hop in range(last // 2, chips // 2 + 1):
                x_step(hop)
        a_start(g)
        if g:
            e_start(g - 1)
    e_start(len(groups) - 1)

    for offset in range(1, rows):
        k_copy(offset).wait_recv()
    for k in range(rows):
        place = jnp.int32(0)
        for i in range(cols):
            place = jnp.where(owner_ref[k * cols + i] == row, i, place)
        flags_ref[pl.ds(k, 1), :] = keeps[k, pl.ds(place, 1), :]
    for n in range(len(x_pieces)):
        for offset in range(chips):
            d_copy(n, offset).wait_recv()
    for g in range(len(groups)):
        for offset in range(chips):
            e_copy(g, offset).wait_recv()

    def left(part, sem):
        copy(part, part, sem, k_recv.at[0], partner, col).wait_send()

    for g in range(len(groups)):
        span = pl.ds(groups[g][0][0], sum(s for _, s in groups[g]))
        left(gathered[g].at[pl.ds(0, cols - 1)], z_send.at[g])
        left(right_ref.at[pl.ds(0, chips - 1), span], x_send.at[g])
        left(right_ref.at[pl.ds(0, chips), span], d_send.at[g])
        pl.when(same)(lambda: left(outbox[g].at[pl.ds(0, chips - 1)], a_send.at[g]))
        pl.when(jnp.logical_not(same))(lambda: left(outbox[g], a_send.at[g]))
        left(left_ref.at[pl.ds(0, chips), span], e_send.at[g])
    left(keeps.at[pl.ds(0, rows - 1)], k_send.at[0])


def multiply(capacity, limit, left_ref, right_ref, flags_ref, owner_ref, tiles_ref, ids_ref, packed, ids, places, sem):
    rows, frames, tile = left_ref.shape
    cols = flags_ref.shape[1]
    row, col = lax.axis_index("row"), lax.axis_index("col")
    total_cols = cols * lax.axis_size("col")
    first_col = col * cols
    for i in range(cols + 1):
        places[i] = 0

    def put(i):
        run = pl.ds(i * RUN, RUN)
        return pltpu.make_async_copy(packed.at[run], tiles_ref.at[run], sem)

    def put_runs(first, end):
        lax.fori_loop(first, end, lambda i, carry: put(i).start(), None)

    start, sent = jnp.int32(0), jnp.int32(0)
    for k in range(rows):
        count = jnp.int32(0)
        for j in range(cols):
            places[count] = j
            count += flags_ref[k, j]
        place = jnp.int32(0)
        for i in range(cols):
            place = jnp.where(owner_ref[k * cols + i] == row, i, place)
        base = (k * cols + place) * total_cols + first_col
        kept = [places[s] for s in range(limit)]
        product = lax.dot_general(
            left_ref[k],
            jnp.concatenate([right_ref[j] for j in kept], axis=1),
            (((0,), (0,)), ((), ())),
            preferred_element_type=jnp.float32,
        ) * (1.0 / frames)
        for s, j in enumerate(kept):
            packed[start + s] = product[:, s * tile : (s + 1) * tile].astype(packed.dtype)
            ids[start + s] = base + j
        start += count
        if k % 4 == 3 and k + 1 < rows:
            ready = lax.div(start, RUN)
            put_runs(sent, ready)
            sent = ready

    def blank(s, carry):
        packed[s] = jnp.zeros_like(packed[s])
        ids[s] = -1
        return carry

    lax.fori_loop(start, capacity, blank, 0)
    put_runs(sent, capacity // RUN)
    for s in range(capacity):
        ids_ref[s] = ids[s]
    pltpu.make_async_copy(packed.at[pl.ds(0, capacity)], tiles_ref, sem).wait()


def shards(series, keep_mask, row_owner):
    frames, tile = series.shape
    row_count, col_count = keep_mask.shape
    rows, cols = lax.axis_size("row"), lax.axis_size("col")
    limit = max(2, 3 * col_count // 8)
    capacity = row_count * limit
    groups = [cut(first, size, PIECES) for first, size in cut(0, frames, GROUPS)]
    sizes = [sum(s for _, s in pieces) for pieces in groups]
    n_z, n_g = sum(len(pieces) for pieces in groups), len(groups)
    chips = rows // 2
    vmem, smem = pl.BlockSpec(memory_space=pltpu.VMEM), pl.BlockSpec(memory_space=pltpu.SMEM)
    dma = pltpu.SemaphoreType.DMA
    left, right, flags = pl.pallas_call(
        functools.partial(move, rows, cols, groups),
        out_shape=(
            jax.ShapeDtypeStruct((rows, frames, tile), jnp.bfloat16),
            jax.ShapeDtypeStruct((rows, frames, tile), jnp.bfloat16),
            jax.ShapeDtypeStruct((rows, col_count), jnp.int32),
        ),
        in_specs=[vmem, vmem, smem],
        out_specs=(vmem, vmem, vmem),
        scratch_shapes=[
            *[pltpu.VMEM((cols, size, tile), jnp.bfloat16) for size in sizes],
            *[pltpu.VMEM((chips, size, tile), jnp.bfloat16) for size in sizes],
            pltpu.VMEM((rows, row_count, col_count), jnp.int32),
            dma((n_g,)),
            dma((n_z, 2, cols // 2)),
            dma((n_g,)),
            dma((n_g, 2, chips // 2)),
            *[dma((n_g,)), dma((n_g, chips))] * 3,
            dma((1,)),
            dma((rows,)),
        ],
        compiler_params=pltpu.CompilerParams(collective_id=0, has_side_effects=True, vmem_limit_bytes=24 * 2**20),
    )(series, keep_mask, row_owner)
    tiles, ids = pl.pallas_call(
        functools.partial(multiply, capacity, limit),
        out_shape=(
            jax.ShapeDtypeStruct((capacity, tile, tile), jnp.bfloat16),
            jax.ShapeDtypeStruct((capacity,), jnp.int32),
        ),
        in_specs=[vmem, vmem, smem, smem],
        out_specs=(pl.BlockSpec(memory_space=pl.ANY), smem),
        scratch_shapes=[
            pltpu.VMEM((capacity + limit, tile, tile), jnp.bfloat16),
            pltpu.SMEM((capacity + limit,), jnp.int32),
            pltpu.SMEM((col_count + 1,), jnp.int32),
            dma(()),
        ],
        compiler_params=pltpu.CompilerParams(vmem_limit_bytes=24 * 2**20),
    )(left, right, flags, row_owner)
    return tiles.reshape(1, 1, capacity, tile, tile), ids.reshape(1, 1, capacity)


def solution(mesh):
    in_specs = (P(None, ("subj", "row", "col")), P(("subj", "row"), "col"), P("subj"))
    out_specs = (P(("subj", "row"), "col", None, None, None), P(("subj", "row"), "col", None))
    return jax.shard_map(shards, mesh=mesh, in_specs=in_specs, out_specs=out_specs, check_vma=False)
```

```python
import functools

import jax
import jax.numpy as jnp
from jax import lax
from jax.experimental import pallas as pl
from jax.experimental.pallas import tpu as pltpu
from jax.sharding import PartitionSpec as P

MESH = pl.DeviceIdType.MESH
EPSILON = 1e-05
RUN = 8
UNIT = 16
GROUPS = 4
LAG = 2
EARLY = 4
X_PIECES = 2
PIECES = 2


def cut(first, size, parts):
    units = size // UNIT
    edges = [first + UNIT * (units * p // parts) for p in range(parts)] + [first + size]
    return [(a, b - a) for a, b in zip(edges[:-1], edges[1:])]


def move(
    rows,
    cols,
    groups,
    series_ref,
    keep_ref,
    owner_ref,
    left_ref,
    right_ref,
    flags_ref,
    *scratch,
):
    gathered, outbox = scratch[: len(groups)], scratch[len(groups) : 2 * len(groups)]
    keeps = scratch[2 * len(groups)]
    z_send, z_recv, x_send, x_recv, d_send, d_recv, a_send, a_recv, e_send, e_recv, k_send, k_recv = scratch[
        2 * len(groups) + 1 :
    ]
    chips = rows // 2
    row, col = lax.axis_index("row"), lax.axis_index("col")
    core, chip = lax.rem(row, 2), lax.div(row, 2)
    up, down = lax.rem(col + 1, cols), lax.rem(col + cols - 1, cols)
    partner = row + 1 - 2 * core

    def chip_at(offset):
        return lax.rem(chip + offset + chips, chips)

    def col_at(offset):
        return lax.rem(col + offset + cols, cols)

    def copy(src, dst, send, recv, to_row, to_col):
        return pltpu.make_async_remote_copy(
            src_ref=src,
            dst_ref=dst,
            send_sem=send,
            recv_sem=recv,
            device_id={"row": to_row, "col": to_col},
            device_id_type=MESH,
        )

    barrier = pltpu.get_barrier_semaphore()
    for to_row in (2 * chip_at(1) + core, 2 * chip_at(-1) + core, partner):
        pl.semaphore_signal(barrier, inc=1, device_id={"row": to_row, "col": col}, device_id_type=MESH)
    for to_col in (up, down):
        pl.semaphore_signal(barrier, inc=1, device_id={"row": row, "col": to_col}, device_id_type=MESH)

    frames = series_ref.shape[0]
    series = series_ref[...]
    centred = series - jnp.sum(series, axis=0, keepdims=True) * (1.0 / frames)
    spread = jnp.sum(centred * centred, axis=0, keepdims=True) * (1.0 / frames)
    scored = (centred * lax.rsqrt(spread + EPSILON)).astype(jnp.bfloat16)
    for g, pieces in enumerate(groups):
        first, size = pieces[0][0], sum(s for _, s in pieces)
        gathered[g][col] = scored[first : first + size]
    right_ref[row] = scored
    keeps[row] = keep_ref[...]

    pl.semaphore_wait(barrier, 5)

    z_pieces = [(g, i, *piece) for g, pieces in enumerate(groups) for i, piece in enumerate(pieces)]
    x_pieces = cut(0, series_ref.shape[0], X_PIECES)

    def z_hops(n, way):
        return cols // 2 if n % 2 == way else cols - 1 - cols // 2

    def x_hops(n, way):
        return chips // 2 if n % 2 == way else chips - 1 - chips // 2

    def z_copy(n, way, hop):
        g, _, first, size = z_pieces[n]
        origin = col_at(1 - hop if way == 0 else hop - 1)
        part = gathered[g].at[origin, pl.ds(first - groups[g][0][0], size)]
        return copy(part, part, z_send.at[g], z_recv.at[n, way, hop - 1], row, up if way == 0 else down)

    def x_copy(n, way, hop):
        first, size = x_pieces[n]
        origin = 2 * chip_at(1 - hop if way == 0 else hop - 1) + core
        part = right_ref.at[origin, pl.ds(first, size)]
        to_row = 2 * chip_at(1 if way == 0 else -1) + core
        return copy(part, part, x_send.at[n], x_recv.at[n, way, hop - 1], to_row, col)

    def d_copy(n, offset):
        first, size = x_pieces[n]
        part = right_ref.at[2 * chip_at(offset) + core, pl.ds(first, size)]
        return copy(part, part, d_send.at[n], d_recv.at[n, offset], partner, col)

    def k_copy(offset):
        return copy(
            keep_ref, keeps.at[row], k_send.at[0], k_recv.at[offset], lax.rem(row + offset, rows), col
        )

    def z_start(g):
        for n, piece in enumerate(z_pieces):
            if piece[0] == g:
                for way in range(2):
                    z_copy(n, way, 1).start()

    def z_step(g, hop):
        for n, piece in enumerate(z_pieces):
            if piece[0] == g:
                for way in range(2):
                    if hop <= z_hops(n, way):
                        z_copy(n, way, hop).wait_recv()
                        if hop < z_hops(n, way):
                            z_copy(n, way, hop + 1).start()

    def x_step(hop):
        for n in range(len(x_pieces)):
            for way in range(2):
                if hop <= x_hops(n, way):
                    x_copy(n, way, hop).wait_recv()
                    if hop < x_hops(n, way):
                        x_copy(n, way, hop + 1).start()
                    d_copy(n, chips - hop if way == 0 else hop).start()

    same = lax.rem(col, 2) == 0
    to_core = lax.rem(row + col, 2)
    offsets = [0] + sorted(range(1, chips), key=lambda o: (min(o, chips - o), o))
    to_up = offsets[::2]

    def a_copy(g, offset):
        first, size = groups[g][0][0], sum(s for _, s in groups[g])
        return copy(
            outbox[g].at[offset],
            left_ref.at[row, pl.ds(first, size)],
            a_send.at[g],
            a_recv.at[g, offset],
            2 * chip_at(offset) + to_core,
            col,
        )

    def picked(offset):
        owner = 2 * chip_at(offset) + to_core
        place = jnp.int32(0)
        for i in range(cols):
            place = jnp.where(owner_ref[row * cols + i] == owner, i, place)
        return place

    def a_start(g):
        first, size = groups[g][0][0], sum(s for _, s in groups[g])
        for offset in offsets[1:] + [0]:
            place = picked(offset)
            if offset:
                outbox[g][offset] = gathered[g][place]
                a_copy(g, offset).start()
            else:

                @pl.when(same)
                def _():
                    left_ref[row, pl.ds(first, size)] = gathered[g][place]

                @pl.when(jnp.logical_not(same))
                def _():
                    outbox[g][offset] = gathered[g][place]
                    a_copy(g, offset).start()

    def e_copy(g, offset):
        first, size = groups[g][0][0], sum(s for _, s in groups[g])
        part = left_ref.at[2 * chip_at(-offset) + to_core, pl.ds(first, size)]
        return copy(part, part, e_send.at[g], e_recv.at[g, offset], row, up if offset in to_up else down)

    def e_start(g):
        for offset in offsets:
            if offset:
                a_copy(g, offset).wait_recv()
            else:

                @pl.when(jnp.logical_not(same))
                def _():
                    a_copy(g, offset).wait_recv()

            e_copy(g, offset).start()

    last = cols // 2
    x_turns = [last * (i + 1) * 3 // (2 * chips) + 1 for i in range(chips // 2)]
    z_start(0)
    for n in range(len(x_pieces)):
        for way in range(2):
            x_copy(n, way, 1).start()
    for n in range(len(x_pieces)):
        d_copy(n, 0).start()
    for turn in range(1, last + LAG * (len(groups) - 1) + 1):
        for g in range(len(groups)):
            hop = turn - LAG * g
            if hop == 0:
                z_start(g)
            if 1 <= hop <= last:
                z_step(g, hop)
        if turn in x_turns:
            x_step(x_turns.index(turn) + 1)
        for g in range(len(groups)):
            if turn - LAG * g == last:
                if g == 0:
                    for n in range(len(x_pieces)):
                        for offset in range(chips):
                            d_copy(n, offset).wait_recv()
                a_start(g)
                if g == 0:
                    for offset in range(1, rows):
                        k_copy(offset).start()
                if g >= EARLY:
                    e_start(g - EARLY)
    for g in range(max(0, len(groups) - EARLY), len(groups)):
        e_start(g)

    for offset in range(1, rows):
        k_copy(offset).wait_recv()
    for k in range(rows):
        place = jnp.int32(0)
        for i in range(cols):
            place = jnp.where(owner_ref[k * cols + i] == row, i, place)
        flags_ref[pl.ds(k, 1), :] = keeps[k, pl.ds(place, 1), :]
    for g in range(len(groups)):
        for offset in range(chips):
            e_copy(g, offset).wait_recv()

    def left(part, sem):
        copy(part, part, sem, k_recv.at[0], partner, col).wait_send()

    for g in range(len(groups)):
        span = pl.ds(groups[g][0][0], sum(s for _, s in groups[g]))
        left(gathered[g].at[pl.ds(0, cols - 1)], z_send.at[g])
        pl.when(same)(lambda: left(outbox[g].at[pl.ds(0, chips - 1)], a_send.at[g]))
        pl.when(jnp.logical_not(same))(lambda: left(outbox[g], a_send.at[g]))
        left(left_ref.at[pl.ds(0, chips), span], e_send.at[g])
    for n, piece in enumerate(x_pieces):
        left(right_ref.at[pl.ds(0, chips - 1), pl.ds(*piece)], x_send.at[n])
        left(right_ref.at[pl.ds(0, chips), pl.ds(*piece)], d_send.at[n])
    left(keeps.at[pl.ds(0, rows - 1)], k_send.at[0])


def multiply(capacity, limit, left_ref, right_ref, flags_ref, owner_ref, tiles_ref, ids_ref, packed, ids, places, sem):
    rows, frames, tile = left_ref.shape
    cols = flags_ref.shape[1]
    row, col = lax.axis_index("row"), lax.axis_index("col")
    total_cols = cols * lax.axis_size("col")
    first_col = col * cols
    for i in range(cols + 1):
        places[i] = 0

    def put(i):
        run = pl.ds(i * RUN, RUN)
        return pltpu.make_async_copy(packed.at[run], tiles_ref.at[run], sem)

    def put_runs(first, end):
        lax.fori_loop(first, end, lambda i, carry: put(i).start(), None)

    start, sent = jnp.int32(0), jnp.int32(0)
    for k in range(rows):
        count = jnp.int32(0)
        for j in range(cols):
            places[count] = j
            count += flags_ref[k, j]
        place = jnp.int32(0)
        for i in range(cols):
            place = jnp.where(owner_ref[k * cols + i] == row, i, place)
        base = (k * cols + place) * total_cols + first_col
        kept = [places[s] for s in range(limit)]
        product = lax.dot_general(
            left_ref[k],
            jnp.concatenate([right_ref[j] for j in kept], axis=1),
            (((0,), (0,)), ((), ())),
            preferred_element_type=jnp.float32,
        ) * (1.0 / frames)
        for s, j in enumerate(kept):
            packed[start + s] = product[:, s * tile : (s + 1) * tile].astype(packed.dtype)
            ids[start + s] = base + j
        start += count
        if k % 4 == 3 and k + 1 < rows:
            ready = lax.div(start, RUN)
            put_runs(sent, ready)
            sent = ready

    def blank(s, carry):
        packed[s] = jnp.zeros_like(packed[s])
        ids[s] = -1
        return carry

    lax.fori_loop(start, capacity, blank, 0)
    put_runs(sent, capacity // RUN)
    for s in range(capacity):
        ids_ref[s] = ids[s]
    pltpu.make_async_copy(packed.at[pl.ds(0, capacity)], tiles_ref, sem).wait()


def shards(series, keep_mask, row_owner):
    frames, tile = series.shape
    row_count, col_count = keep_mask.shape
    rows, cols = lax.axis_size("row"), lax.axis_size("col")
    limit = max(2, 3 * col_count // 8)
    capacity = row_count * limit
    groups = [cut(first, size, PIECES) for first, size in cut(0, frames, GROUPS)]
    sizes = [sum(s for _, s in pieces) for pieces in groups]
    n_z, n_g = sum(len(pieces) for pieces in groups), len(groups)
    chips = rows // 2
    vmem, smem = pl.BlockSpec(memory_space=pltpu.VMEM), pl.BlockSpec(memory_space=pltpu.SMEM)
    dma = pltpu.SemaphoreType.DMA
    left, right, flags = pl.pallas_call(
        functools.partial(move, rows, cols, groups),
        out_shape=(
            jax.ShapeDtypeStruct((rows, frames, tile), jnp.bfloat16),
            jax.ShapeDtypeStruct((rows, frames, tile), jnp.bfloat16),
            jax.ShapeDtypeStruct((rows, col_count), jnp.int32),
        ),
        in_specs=[vmem, vmem, smem],
        out_specs=(vmem, vmem, vmem),
        scratch_shapes=[
            *[pltpu.VMEM((cols, size, tile), jnp.bfloat16) for size in sizes],
            *[pltpu.VMEM((chips, size, tile), jnp.bfloat16) for size in sizes],
            pltpu.VMEM((rows, row_count, col_count), jnp.int32),
            dma((n_g,)),
            dma((n_z, 2, cols // 2)),
            dma((X_PIECES,)),
            dma((X_PIECES, 2, chips // 2)),
            dma((X_PIECES,)),
            dma((X_PIECES, chips)),
            *[dma((n_g,)), dma((n_g, chips))] * 2,
            dma((1,)),
            dma((rows,)),
        ],
        compiler_params=pltpu.CompilerParams(collective_id=0, has_side_effects=True, vmem_limit_bytes=24 * 2**20),
    )(series, keep_mask, row_owner)
    tiles, ids = pl.pallas_call(
        functools.partial(multiply, capacity, limit),
        out_shape=(
            jax.ShapeDtypeStruct((capacity, tile, tile), jnp.bfloat16),
            jax.ShapeDtypeStruct((capacity,), jnp.int32),
        ),
        in_specs=[vmem, vmem, smem, smem],
        out_specs=(pl.BlockSpec(memory_space=pl.ANY), smem),
        scratch_shapes=[
            pltpu.VMEM((capacity + limit, tile, tile), jnp.bfloat16),
            pltpu.SMEM((capacity + limit,), jnp.int32),
            pltpu.SMEM((col_count + 1,), jnp.int32),
            dma(()),
        ],
        compiler_params=pltpu.CompilerParams(vmem_limit_bytes=24 * 2**20),
    )(left, right, flags, row_owner)
    return tiles.reshape(1, 1, capacity, tile, tile), ids.reshape(1, 1, capacity)


def solution(mesh):
    in_specs = (P(None, ("subj", "row", "col")), P(("subj", "row"), "col"), P("subj"))
    out_specs = (P(("subj", "row"), "col", None, None, None), P(("subj", "row"), "col", None))
    return jax.shard_map(shards, mesh=mesh, in_specs=in_specs, out_specs=out_specs, check_vma=False)
```

```python
import functools

import jax
import jax.numpy as jnp
from jax import lax
from jax.experimental import pallas as pl
from jax.experimental.pallas import tpu as pltpu
from jax.sharding import PartitionSpec as P

MESH = pl.DeviceIdType.MESH
EPSILON = 1e-05
RUN = 8
UNIT = 16
GROUPS = 4
LAG = 2
X_PIECES = 2
PIECES = 2


def cut(first, size, parts):
    units = size // UNIT
    edges = [first + UNIT * (units * p // parts) for p in range(parts)] + [first + size]
    return [(a, b - a) for a, b in zip(edges[:-1], edges[1:])]


def move(
    rows,
    cols,
    groups,
    series_ref,
    keep_ref,
    owner_ref,
    left_ref,
    right_ref,
    flags_ref,
    *scratch,
):
    gathered, outbox = scratch[: len(groups)], scratch[len(groups) : 2 * len(groups)]
    keeps = scratch[2 * len(groups)]
    z_send, z_recv, x_send, x_recv, d_send, d_recv, a_send, a_recv, e_send, e_recv, k_send, k_recv = scratch[
        2 * len(groups) + 1 :
    ]
    chips = rows // 2
    row, col = lax.axis_index("row"), lax.axis_index("col")
    core, chip = lax.rem(row, 2), lax.div(row, 2)
    up, down = lax.rem(col + 1, cols), lax.rem(col + cols - 1, cols)
    partner = row + 1 - 2 * core

    def chip_at(offset):
        return lax.rem(chip + offset + chips, chips)

    def col_at(offset):
        return lax.rem(col + offset + cols, cols)

    def copy(src, dst, send, recv, to_row, to_col):
        return pltpu.make_async_remote_copy(
            src_ref=src,
            dst_ref=dst,
            send_sem=send,
            recv_sem=recv,
            device_id={"row": to_row, "col": to_col},
            device_id_type=MESH,
        )

    barrier = pltpu.get_barrier_semaphore()
    for offset in range(1, rows):
        pl.semaphore_signal(
            barrier, inc=1, device_id={"row": lax.rem(row + offset, rows), "col": col}, device_id_type=MESH
        )
    for to_col in (up, down):
        pl.semaphore_signal(barrier, inc=1, device_id={"row": row, "col": to_col}, device_id_type=MESH)

    frames = series_ref.shape[0]
    series = series_ref[...]
    centred = series - jnp.sum(series, axis=0, keepdims=True) * (1.0 / frames)
    spread = jnp.sum(centred * centred, axis=0, keepdims=True) * (1.0 / frames)
    scored = (centred * lax.rsqrt(spread + EPSILON)).astype(jnp.bfloat16)
    for g, pieces in enumerate(groups):
        first, size = pieces[0][0], sum(s for _, s in pieces)
        gathered[g][col] = scored[first : first + size]
    right_ref[row] = scored
    keeps[row] = keep_ref[...]

    pl.semaphore_wait(barrier, rows + 1)

    z_pieces = [(g, i, *piece) for g, pieces in enumerate(groups) for i, piece in enumerate(pieces)]
    x_pieces = cut(0, series_ref.shape[0], X_PIECES)

    def z_hops(n, way):
        return cols // 2 if n % 2 == way else cols - 1 - cols // 2

    def x_hops(n, way):
        return chips // 2 if n % 2 == way else chips - 1 - chips // 2

    def z_copy(n, way, hop):
        g, _, first, size = z_pieces[n]
        origin = col_at(1 - hop if way == 0 else hop - 1)
        part = gathered[g].at[origin, pl.ds(first - groups[g][0][0], size)]
        return copy(part, part, z_send.at[g], z_recv.at[n, way, hop - 1], row, up if way == 0 else down)

    def x_copy(n, way, hop):
        first, size = x_pieces[n]
        origin = 2 * chip_at(1 - hop if way == 0 else hop - 1) + core
        part = right_ref.at[origin, pl.ds(first, size)]
        to_row = 2 * chip_at(1 if way == 0 else -1) + core
        return copy(part, part, x_send.at[n], x_recv.at[n, way, hop - 1], to_row, col)

    def d_copy(n, offset):
        first, size = x_pieces[n]
        part = right_ref.at[2 * chip_at(offset) + core, pl.ds(first, size)]
        return copy(part, part, d_send.at[n], d_recv.at[n, offset], partner, col)

    def k_copy(offset):
        return copy(
            keep_ref, keeps.at[row], k_send.at[0], k_recv.at[offset], lax.rem(row + offset, rows), col
        )

    def z_start(g):
        for n, piece in enumerate(z_pieces):
            if piece[0] == g:
                for way in range(2):
                    z_copy(n, way, 1).start()

    def z_step(g, hop):
        for n, piece in enumerate(z_pieces):
            if piece[0] == g:
                for way in range(2):
                    if hop <= z_hops(n, way):
                        z_copy(n, way, hop).wait_recv()
                        if hop < z_hops(n, way):
                            z_copy(n, way, hop + 1).start()

    def x_step(hop):
        for n in range(len(x_pieces)):
            for way in range(2):
                if hop <= x_hops(n, way):
                    x_copy(n, way, hop).wait_recv()
                    if hop < x_hops(n, way):
                        x_copy(n, way, hop + 1).start()
                    d_copy(n, chips - hop if way == 0 else hop).start()

    same = lax.rem(col, 2) == 0
    to_core = lax.rem(row + col, 2)
    offsets = [0] + sorted(range(1, chips), key=lambda o: (min(o, chips - o), o))
    to_up = offsets[::2]

    def a_copy(g, offset):
        first, size = groups[g][0][0], sum(s for _, s in groups[g])
        return copy(
            outbox[g].at[offset],
            left_ref.at[row, pl.ds(first, size)],
            a_send.at[g],
            a_recv.at[g, offset],
            2 * chip_at(offset) + to_core,
            col,
        )

    def picked(offset):
        owner = 2 * chip_at(offset) + to_core
        place = jnp.int32(0)
        for i in range(cols):
            place = jnp.where(owner_ref[row * cols + i] == owner, i, place)
        return place

    def a_start(g):
        first, size = groups[g][0][0], sum(s for _, s in groups[g])
        for offset in offsets[1:] + [0]:
            place = picked(offset)
            if offset:
                outbox[g][offset] = gathered[g][place]
                a_copy(g, offset).start()
            else:

                @pl.when(same)
                def _():
                    left_ref[row, pl.ds(first, size)] = gathered[g][place]

                @pl.when(jnp.logical_not(same))
                def _():
                    outbox[g][offset] = gathered[g][place]
                    a_copy(g, offset).start()

    def e_copy(g, offset):
        first, size = groups[g][0][0], sum(s for _, s in groups[g])
        part = left_ref.at[2 * chip_at(-offset) + to_core, pl.ds(first, size)]
        return copy(part, part, e_send.at[g], e_recv.at[g, offset], row, up if offset in to_up else down)

    def e_start(g):
        for offset in offsets:
            if offset:
                a_copy(g, offset).wait_recv()
            else:

                @pl.when(jnp.logical_not(same))
                def _():
                    a_copy(g, offset).wait_recv()

            e_copy(g, offset).start()

    last = cols // 2
    z_start(0)
    for n in range(len(x_pieces)):
        for way in range(2):
            x_copy(n, way, 1).start()
    for offset in range(1, rows):
        k_copy(offset).start()
    for n in range(len(x_pieces)):
        d_copy(n, 0).start()
    for turn in range(1, last + LAG * (len(groups) - 1) + 1):
        for g in range(len(groups)):
            hop = turn - LAG * g
            if hop == 0:
                z_start(g)
            if 1 <= hop <= last:
                z_step(g, hop)
        if turn <= last and turn % 2 == 0:
            x_step(turn // 2)
        for g in range(len(groups)):
            if turn - LAG * g == last:
                a_start(g)
    for g in range(len(groups)):
        e_start(g)

    for offset in range(1, rows):
        k_copy(offset).wait_recv()
    for k in range(rows):
        place = jnp.int32(0)
        for i in range(cols):
            place = jnp.where(owner_ref[k * cols + i] == row, i, place)
        flags_ref[pl.ds(k, 1), :] = keeps[k, pl.ds(place, 1), :]
    for n in range(len(x_pieces)):
        for offset in range(chips):
            d_copy(n, offset).wait_recv()
    for g in range(len(groups)):
        for offset in range(chips):
            e_copy(g, offset).wait_recv()

    def left(part, sem):
        copy(part, part, sem, k_recv.at[0], partner, col).wait_send()

    for g in range(len(groups)):
        span = pl.ds(groups[g][0][0], sum(s for _, s in groups[g]))
        left(gathered[g].at[pl.ds(0, cols - 1)], z_send.at[g])
        pl.when(same)(lambda: left(outbox[g].at[pl.ds(0, chips - 1)], a_send.at[g]))
        pl.when(jnp.logical_not(same))(lambda: left(outbox[g], a_send.at[g]))
        left(left_ref.at[pl.ds(0, chips), span], e_send.at[g])
    for n, piece in enumerate(x_pieces):
        left(right_ref.at[pl.ds(0, chips - 1), pl.ds(*piece)], x_send.at[n])
        left(right_ref.at[pl.ds(0, chips), pl.ds(*piece)], d_send.at[n])
    left(keeps.at[pl.ds(0, rows - 1)], k_send.at[0])


def multiply(capacity, limit, left_ref, right_ref, flags_ref, owner_ref, tiles_ref, ids_ref, packed, ids, places, sem):
    rows, frames, tile = left_ref.shape
    cols = flags_ref.shape[1]
    row, col = lax.axis_index("row"), lax.axis_index("col")
    total_cols = cols * lax.axis_size("col")
    first_col = col * cols
    for i in range(cols + 1):
        places[i] = 0

    def put(i):
        run = pl.ds(i * RUN, RUN)
        return pltpu.make_async_copy(packed.at[run], tiles_ref.at[run], sem)

    def put_runs(first, end):
        lax.fori_loop(first, end, lambda i, carry: put(i).start(), None)

    start, sent = jnp.int32(0), jnp.int32(0)
    for k in range(rows):
        count = jnp.int32(0)
        for j in range(cols):
            places[count] = j
            count += flags_ref[k, j]
        place = jnp.int32(0)
        for i in range(cols):
            place = jnp.where(owner_ref[k * cols + i] == row, i, place)
        base = (k * cols + place) * total_cols + first_col
        kept = [places[s] for s in range(limit)]
        product = lax.dot_general(
            left_ref[k],
            jnp.concatenate([right_ref[j] for j in kept], axis=1),
            (((0,), (0,)), ((), ())),
            preferred_element_type=jnp.float32,
        ) * (1.0 / frames)
        for s, j in enumerate(kept):
            packed[start + s] = product[:, s * tile : (s + 1) * tile].astype(packed.dtype)
            ids[start + s] = base + j
        start += count
        if k % 4 == 3 and k + 1 < rows:
            ready = lax.div(start, RUN)
            put_runs(sent, ready)
            sent = ready

    def blank(s, carry):
        packed[s] = jnp.zeros_like(packed[s])
        ids[s] = -1
        return carry

    lax.fori_loop(start, capacity, blank, 0)
    put_runs(sent, capacity // RUN)
    for s in range(capacity):
        ids_ref[s] = ids[s]
    pltpu.make_async_copy(packed.at[pl.ds(0, capacity)], tiles_ref, sem).wait()


def shards(series, keep_mask, row_owner):
    frames, tile = series.shape
    row_count, col_count = keep_mask.shape
    rows, cols = lax.axis_size("row"), lax.axis_size("col")
    limit = max(2, 3 * col_count // 8)
    capacity = row_count * limit
    groups = [cut(first, size, PIECES) for first, size in cut(0, frames, GROUPS)]
    sizes = [sum(s for _, s in pieces) for pieces in groups]
    n_z, n_g = sum(len(pieces) for pieces in groups), len(groups)
    chips = rows // 2
    vmem, smem = pl.BlockSpec(memory_space=pltpu.VMEM), pl.BlockSpec(memory_space=pltpu.SMEM)
    dma = pltpu.SemaphoreType.DMA
    left, right, flags = pl.pallas_call(
        functools.partial(move, rows, cols, groups),
        out_shape=(
            jax.ShapeDtypeStruct((rows, frames, tile), jnp.bfloat16),
            jax.ShapeDtypeStruct((rows, frames, tile), jnp.bfloat16),
            jax.ShapeDtypeStruct((rows, col_count), jnp.int32),
        ),
        in_specs=[vmem, vmem, smem],
        out_specs=(vmem, vmem, vmem),
        scratch_shapes=[
            *[pltpu.VMEM((cols, size, tile), jnp.bfloat16) for size in sizes],
            *[pltpu.VMEM((chips, size, tile), jnp.bfloat16) for size in sizes],
            pltpu.VMEM((rows, row_count, col_count), jnp.int32),
            dma((n_g,)),
            dma((n_z, 2, cols // 2)),
            dma((X_PIECES,)),
            dma((X_PIECES, 2, chips // 2)),
            dma((X_PIECES,)),
            dma((X_PIECES, chips)),
            *[dma((n_g,)), dma((n_g, chips))] * 2,
            dma((1,)),
            dma((rows,)),
        ],
        compiler_params=pltpu.CompilerParams(collective_id=0, has_side_effects=True, vmem_limit_bytes=24 * 2**20),
    )(series, keep_mask, row_owner)
    tiles, ids = pl.pallas_call(
        functools.partial(multiply, capacity, limit),
        out_shape=(
            jax.ShapeDtypeStruct((capacity, tile, tile), jnp.bfloat16),
            jax.ShapeDtypeStruct((capacity,), jnp.int32),
        ),
        in_specs=[vmem, vmem, smem, smem],
        out_specs=(pl.BlockSpec(memory_space=pl.ANY), smem),
        scratch_shapes=[
            pltpu.VMEM((capacity + limit, tile, tile), jnp.bfloat16),
            pltpu.SMEM((capacity + limit,), jnp.int32),
            pltpu.SMEM((col_count + 1,), jnp.int32),
            dma(()),
        ],
        compiler_params=pltpu.CompilerParams(vmem_limit_bytes=24 * 2**20),
    )(left, right, flags, row_owner)
    return tiles.reshape(1, 1, capacity, tile, tile), ids.reshape(1, 1, capacity)


def solution(mesh):
    in_specs = (P(None, ("subj", "row", "col")), P(("subj", "row"), "col"), P("subj"))
    out_specs = (P(("subj", "row"), "col", None, None, None), P(("subj", "row"), "col", None))
    return jax.shard_map(shards, mesh=mesh, in_specs=in_specs, out_specs=out_specs, check_vma=False)
```
